8 devices in a mesh: rows: 2 (over z, y), terms: 4 (over x, core).
Axes of the slice: x: 2, y: 2, z: 1, core: 2. Of those that a mesh axis runs over, the one named last changes fastest.
Arguments:
- psi_init: float32 [768, 4, 4, 768], P(('rows', 'terms'))
- left_env: bfloat16 [24, 768, 768], P('terms', 'rows')
- two_site: bfloat16 [24, 16, 16], P('terms')
- right_env: bfloat16 [24, 768, 768], P('terms')
Outputs:
- output 1: float32 [7, 768, 4, 4, 768], P(None, ('rows', 'terms'))
- output 2: float32 [6], replicated
- output 3: float32 [6], replicated
All inputs are finite; a program needn't handle non-finite values.
Results may differ from the reference program's by a relative error of at most 0.02.
Values are sent between devices in bfloat16 or wider.
A program may use at most 1 GiB of HBM per device.

```python
import jax
import jax.numpy as jnp
from jax import lax

BOND = 768
PHYS = 4
TERMS = 24
STEPS = 6


def sym_normal(base_key, num_mats, mat_size):
    raw_mat = jax.random.normal(base_key, (num_mats, mat_size, mat_size), jnp.float32)
    return (raw_mat + jnp.swapaxes(raw_mat, 1, 2)) * (2.0 * mat_size) ** -0.5


def setup_inputs(seed: int = 0) -> dict:
    base_key = jax.random.key(seed)
    k_psi, k_left, k_two, k_right = jax.random.split(base_key, 4)
    phys_pair = PHYS * PHYS
    psi_init = jax.random.normal(k_psi, (BOND, PHYS, PHYS, BOND), jnp.float32)
    left_env = (sym_normal(k_left, TERMS, BOND) * TERMS ** -0.5).astype(jnp.bfloat16)
    two_site = sym_normal(k_two, TERMS, phys_pair).astype(jnp.bfloat16)
    right_env = sym_normal(k_right, TERMS, BOND).astype(jnp.bfloat16)
    return {"psi_init": psi_init, "left_env": left_env, "two_site": two_site, "right_env": right_env}


def reference(psi_init, left_env, two_site, right_env):
    bond_dim = psi_init.shape[0]
    phys_pair = psi_init.shape[1] * psi_init.shape[2]
    elem_count = psi_init.size

    def inner_mean(x_vec, y_vec):
        return jnp.sum(x_vec * y_vec) / elem_count

    def matvec(cur_vec):
        flat_vec = cur_vec.astype(jnp.bfloat16).reshape(bond_dim, phys_pair * bond_dim)

        def term_step(acc_sum, term_mats):
            left_k, two_k, right_k = term_mats
            left_out = jnp.dot(left_k, flat_vec, preferred_element_type=jnp.float32)
            left_out = left_out.astype(jnp.bfloat16).reshape(bond_dim, phys_pair, bond_dim)
            phys_out = jnp.einsum("aqc,pq->apc", left_out.astype(jnp.float32), two_k.astype(jnp.float32)).astype(jnp.bfloat16)
            right_out = jnp.dot(phys_out.reshape(bond_dim * phys_pair, bond_dim), right_k.T, preferred_element_type=jnp.float32)
            return acc_sum + right_out.reshape(bond_dim, phys_pair, bond_dim), None

        zero_acc = jnp.zeros((bond_dim, phys_pair, bond_dim), jnp.float32)
        sigma_sum = lax.scan(term_step, zero_acc, (left_env, two_site, right_env))[0]
        return sigma_sum.reshape(cur_vec.shape)

    cur_vec = psi_init / jnp.sqrt(inner_mean(psi_init, psi_init))
    prev_vec = cur_vec
    beta_prev = None
    vectors = [cur_vec]
    alpha_list = []
    beta_list = []
    for step_idx in range(STEPS):
        w_vec = matvec(cur_vec)
        alpha_j = inner_mean(w_vec, cur_vec)
        w_vec = w_vec - alpha_j * cur_vec
        if step_idx > 0:
            w_vec = w_vec - beta_prev * prev_vec
        beta_j = jnp.sqrt(inner_mean(w_vec, w_vec))
        prev_vec = cur_vec
        cur_vec = w_vec / beta_j
        beta_prev = beta_j
        vectors.append(cur_vec)
        alpha_list.append(alpha_j)
        beta_list.append(beta_j)
    return (jnp.stack(vectors), jnp.stack(alpha_list), jnp.stack(beta_list))
```

```python
import functools

import jax
import jax.numpy as jnp
from jax import lax
from jax.experimental import pallas as pl
from jax.experimental.pallas import tpu as pltpu
from jax.sharding import PartitionSpec as P

STEPS = 6
MESH = pl.DeviceIdType.MESH
BF = jnp.bfloat16
F32 = jnp.float32
LANE = 128
SEND_O, SEND_F, SEND_P, FWD_D, FWD_PO, FWD_PF, FWD_PD = range(7)
R_OWN, R_X, R_Y, R_PX, R_PY = range(5)


def lanczos_kernel(psi_ref, left_ref, kron_ref, right_ref, out_ref, ab_ref, rbuf,
                   vecs, uvec, lvm, kvm, rvm, xbuf, ybuf, sums, beta_s,
                   load_sem, rload_sem, out_sem, u_send, u_recv, r_send, r_recv,
                   l_send, l_recv, s_send, s_recv):
    group_terms, _, bond = left_ref.shape
    phys, slab, _ = psi_ref.shape
    chunks = bond // LANE
    groups = 4
    elem_count = phys * bond * bond
    half_terms = group_terms // 2

    r = lax.axis_index("rows")
    t = lax.axis_index("terms")
    c = t % 2
    x = t // 2
    me = r * 4 + t
    xn = (1 - x) * 2 + c
    part_t = t + 1 - 2 * c
    xnp = xn + 1 - 2 * c
    f_dev = (r + (1 - c) * (1 - 2 * r), t + c * (xn - t))
    o_dev = (r + c * (1 - 2 * r), t + (1 - c) * (xn - t))
    d_dev = (1 - r, xn)
    p_dev = (r, part_t)
    y_dev = (1 - r, t)
    x_dev = (r, xn)

    def block_of(dev):
        return dev[0] * 4 + dev[1]

    def rows_of(block):
        return pl.ds(pl.multiple_of(block * slab, 16), slab)

    def remote(src, dst, ssem, rsem, dev):
        return pltpu.make_async_remote_copy(src_ref=src, dst_ref=dst, send_sem=ssem, recv_sem=rsem,
                                            device_id=dev, device_id_type=MESH)

    def u_copy(kind, ci):
        block = {SEND_O: block_of((r, t)), SEND_F: block_of((r, t)), SEND_P: block_of((r, t)),
                 FWD_D: block_of(o_dev), FWD_PO: block_of(o_dev),
                 FWD_PF: block_of(f_dev), FWD_PD: block_of(d_dev)}[kind]
        dev = {SEND_O: o_dev, SEND_F: f_dev, SEND_P: p_dev, FWD_D: f_dev,
               FWD_PO: p_dev, FWD_PF: p_dev, FWD_PD: p_dev}[kind]
        ref = uvec.at[ci, :, rows_of(block), :]
        return remote(ref, ref, u_send.at[kind, ci], u_recv.at[kind, ci], dev)

    def r_copy(kind, ci):
        rows = pl.ds(pl.multiple_of(ci * LANE, LANE), LANE)
        mine = pl.ds(r * half_terms, half_terms)
        other = pl.ds((1 - r) * half_terms, half_terms)
        src, dst, dev = {
            R_OWN: (right_ref.at[:, rows, :], rbuf.at[0, :, rows, :], p_dev),
            R_X: (right_ref.at[mine, rows, :], rbuf.at[1, mine, rows, :], x_dev),
            R_Y: (rbuf.at[1, mine, rows, :], rbuf.at[1, mine, rows, :], y_dev),
            R_PX: (rbuf.at[1, mine, rows, :], rbuf.at[2, mine, rows, :], p_dev),
            R_PY: (rbuf.at[1, other, rows, :], rbuf.at[2, other, rows, :], p_dev),
        }[kind]
        return remote(src, dst, r_send.at[kind, ci], r_recv.at[kind, ci], dev)

    def l_copy(g):
        tgt = (part_t, xn, xnp)[g]
        return remote(left_ref.at[:, rows_of(tgt), :], lvm.at[g + 1], l_send.at[g], l_recv.at[g], (r, tgt))

    def r_load(ci, kg, slot):
        rows = pl.ds(pl.multiple_of(ci * LANE, LANE), LANE)

        @pl.when(kg == 0)
        def _():
            pltpu.make_async_copy(right_ref.at[:, rows, :], rvm.at[slot], rload_sem.at[slot]).start()

        @pl.when(kg != 0)
        def _():
            pltpu.make_async_copy(rbuf.at[jnp.maximum(kg - 1, 0), :, rows, :], rvm.at[slot], rload_sem.at[slot]).start()

    def r_load_wait(slot):
        pltpu.make_async_copy(right_ref.at[:, pl.ds(0, LANE), :], rvm.at[slot], rload_sem.at[slot]).wait()

    def sum_copy(kind, rel):
        tgt = (me + rel) % 8
        ref = sums.at[kind, me]
        return remote(ref, ref, s_send.at[kind, rel - 1], s_recv.at[kind, rel - 1], (tgt // 4, tgt % 4))

    def all_mean(kind, partial):
        sums[kind, pl.ds(me, 1)] = partial[None]
        for rel in range(1, 8):
            sum_copy(kind, rel).start()
        for rel in range(1, 8):
            sum_copy(kind, rel).wait()
        tile = jnp.sum(sums[kind], axis=0)
        total = jnp.sum(jnp.sum(tile, axis=0, keepdims=True), axis=1, keepdims=True)
        return total / elem_count

    def fold_tiles(arr):
        acc = jnp.zeros((8, LANE), F32)
        for i in range(slab // 8):
            for j in range(bond // LANE):
                acc = acc + arr[i * 8:i * 8 + 8, j * LANE:j * LANE + LANE]
        return acc

    def norm_and_pack(slot, scale, pack):
        def one_chunk(ci):
            lanes = pl.ds(pl.multiple_of(ci * LANE, LANE), LANE)

            def one_q(qp, _):
                for h in range(2):
                    val = vecs[slot, 2 * qp + h, :, lanes] * scale
                    vecs[slot, 2 * qp + h, :, lanes] = val
                    if pack:
                        uvec[ci, qp, rows_of(me), h * LANE:(h + 1) * LANE] = val.astype(BF)
                return 0
            lax.fori_loop(0, phys // 2, one_q, 0)
        if pack:
            one_chunk(0)
            one_chunk(1)
            for kind in (SEND_O, SEND_F, SEND_P):
                u_copy(kind, 0).start()
            u_copy(SEND_O, 1).start()

            def rest(ci, _):
                one_chunk(ci)
                return 0
            lax.fori_loop(2, chunks, rest, 0)
        else:
            def every(ci, _):
                one_chunk(ci)
                return 0
            lax.fori_loop(0, chunks, every, 0)

    def out_copy(slot, idx):
        return pltpu.make_async_copy(vecs.at[slot], out_ref.at[idx], out_sem.at[slot])

    barrier = pltpu.get_barrier_semaphore()
    for rel in range(1, 8):
        tgt = (me + rel) % 8
        pl.semaphore_signal(barrier, inc=1, device_id=(tgt // 4, tgt % 4), device_id_type=MESH)
    psi_load = pltpu.make_async_copy(psi_ref, vecs.at[0], load_sem.at[0])
    psi_load.start()
    kron_load = pltpu.make_async_copy(kron_ref, kvm, load_sem.at[1])
    kron_load.start()
    own_left = pltpu.make_async_copy(left_ref.at[:, rows_of(t), :], lvm.at[0], load_sem.at[2])
    own_left.start()
    pl.semaphore_wait(barrier, 7)
    r_copy(R_X, 0).start()
    r_copy(R_OWN, 0).start()
    for g in range(3):
        l_copy(g).start()
    r_load(0, 0, 0)
    psi_load.wait()

    def sq_q(q, acc):
        val = vecs[0, q]
        return acc + fold_tiles(val * val)
    norm = jnp.sqrt(all_mean(1, lax.fori_loop(0, phys, sq_q, jnp.zeros((8, LANE), F32))))
    norm_and_pack(0, 1.0 / norm, True)
    r_copy(R_X, 1).start()
    r_copy(R_OWN, 1).start()
    out_copy(0, 0).start()
    r_copy(R_X, 0).wait_recv()
    r_copy(R_Y, 0).start()
    r_copy(R_PX, 0).start()
    beta_s[...] = jnp.zeros_like(beta_s)
    kron_load.wait()
    own_left.wait()

    def step_body(step, _):
        cur = step % 3
        prev = (step + 2) % 3
        nxt = (step + 1) % 3

        @pl.when(step >= 2)
        def _():
            out_copy(nxt, step - 2).wait()

        def zero_q(q, _):
            vecs[nxt, q] = jnp.zeros((slab, bond), F32)
            return 0
        lax.fori_loop(0, phys, zero_q, 0)

        u_copy(SEND_O, 0).wait_recv()
        u_copy(FWD_D, 0).start()
        u_copy(FWD_PO, 0).start()
        u_copy(SEND_F, 1).start()
        u_copy(SEND_P, 1).start()

        @pl.when(step == 0)
        def _():
            r_copy(R_Y, 0).wait_recv()
            r_copy(R_PY, 0).start()
        u_copy(SEND_F, 0).wait_recv()
        u_copy(FWD_PF, 0).start()
        u_copy(FWD_D, 0).wait_recv()
        u_copy(FWD_PD, 0).start()

        def iteration(it, _):
            ci = it // groups
            kg = it % groups
            slot = it % 2
            first = step == 0

            @pl.when(kg == 0)
            def _():
                for kind in (SEND_P, FWD_PO, FWD_PF, FWD_PD):
                    u_copy(kind, ci).wait_recv()

                @pl.when(first)
                def _():
                    r_copy(R_OWN, ci).wait_recv()

                    @pl.when(ci + 2 < chunks)
                    def _():
                        r_copy(R_X, ci + 2).start()
                        r_copy(R_OWN, ci + 2).start()

                @pl.when(ci + 2 < chunks)
                def _():
                    u_copy(SEND_O, ci + 2).start()

            @pl.when(jnp.logical_and(kg == 1, ci + 1 < chunks))
            def _():
                @pl.when(first)
                def _():
                    r_copy(R_X, ci + 1).wait_recv()
                    r_copy(R_Y, ci + 1).start()
                    r_copy(R_PX, ci + 1).start()
                u_copy(SEND_O, ci + 1).wait_recv()
                u_copy(FWD_D, ci + 1).start()
                u_copy(FWD_PO, ci + 1).start()

                @pl.when(ci + 2 < chunks)
                def _():
                    u_copy(SEND_F, ci + 2).start()
                    u_copy(SEND_P, ci + 2).start()

            @pl.when(jnp.logical_and(kg == 2, ci + 1 < chunks))
            def _():
                u_copy(SEND_F, ci + 1).wait_recv()
                u_copy(FWD_PF, ci + 1).start()

            @pl.when(jnp.logical_and(kg == 3, ci + 1 < chunks))
            def _():
                u_copy(FWD_D, ci + 1).wait_recv()
                u_copy(FWD_PD, ci + 1).start()

                @pl.when(first)
                def _():
                    r_copy(R_Y, ci + 1).wait_recv()
                    r_copy(R_PY, ci + 1).start()

            @pl.when(jnp.logical_and(first, kg == 2))
            def _():
                r_copy(R_PX, ci).wait_recv()
                r_copy(R_PY, ci).wait_recv()

            @pl.when(jnp.logical_and(first, ci == 0))
            def _():
                for g in range(3):
                    @pl.when(kg == g + 1)
                    def _():
                        l_copy(g).wait_recv()

            r_load_wait(slot)
            last = jnp.logical_and(step == STEPS - 1, it == groups * chunks - 1)

            @pl.when(jnp.logical_not(last))
            def _():
                nit = (it + 1) % (groups * chunks)
                r_load(nit // groups, nit % groups, 1 - slot)

            left = lvm[kg].reshape(group_terms * slab, bond)
            for qp in range(phys // 2):
                o = jnp.dot(left, uvec[ci, qp], preferred_element_type=F32).astype(BF)
                xbuf[2 * qp] = o[:, :LANE]
                xbuf[2 * qp + 1] = o[:, LANE:]
            for k in range(group_terms):
                for ap in range(slab // 32):
                    r0 = k * slab + ap * 32
                    xa = xbuf[:, r0:r0 + 16, :].reshape(16 * phys, LANE)
                    xb = xbuf[:, r0 + 16:r0 + 32, :].reshape(16 * phys, LANE)
                    y = jnp.dot(kvm[kg, k], jnp.concatenate([xa, xb], axis=1), preferred_element_type=F32).astype(BF)
                    ybuf[:, ap * 32:ap * 32 + 16, k * LANE:(k + 1) * LANE] = y[:, :LANE].reshape(phys, 16, LANE)
                    ybuf[:, ap * 32 + 16:ap * 32 + 32, k * LANE:(k + 1) * LANE] = y[:, LANE:].reshape(phys, 16, LANE)
            vecs[nxt] += jnp.dot(ybuf[...].reshape(phys * slab, group_terms * LANE),
                                 rvm[slot].reshape(group_terms * LANE, bond),
                                 preferred_element_type=F32).reshape(phys, slab, bond)
            return 0
        lax.fori_loop(0, groups * chunks, iteration, 0)

        def drain(ci, _):
            for kind in range(7):
                u_copy(kind, ci).wait_send()

            @pl.when(step == 0)
            def _():
                for kind in range(5):
                    r_copy(kind, ci).wait_send()
            return 0
        lax.fori_loop(0, chunks, drain, 0)

        @pl.when(step == 0)
        def _():
            for g in range(3):
                l_copy(g).wait_send()

        def dot_q(q, acc):
            return acc + fold_tiles(vecs[nxt, q] * vecs[cur, q])
        alpha = all_mean(0, lax.fori_loop(0, phys, dot_q, jnp.zeros((8, LANE), F32)))
        beta_prev = beta_s[0:1, 0:1]

        @pl.when(step == 0)
        def _():
            def upd_q(q, _):
                vecs[nxt, q] = vecs[nxt, q] - alpha * vecs[cur, q]
                return 0
            lax.fori_loop(0, phys, upd_q, 0)

        @pl.when(step > 0)
        def _():
            def upd_q(q, _):
                vecs[nxt, q] = vecs[nxt, q] - alpha * vecs[cur, q] - beta_prev * vecs[prev, q]
                return 0
            lax.fori_loop(0, phys, upd_q, 0)

        def sq_nxt(q, acc):
            val = vecs[nxt, q]
            return acc + fold_tiles(val * val)
        beta = jnp.sqrt(all_mean(1, lax.fori_loop(0, phys, sq_nxt, jnp.zeros((8, LANE), F32))))
        beta_s[...] = jnp.broadcast_to(beta, beta_s.shape)
        ab_ref[pl.ds(step, 1), :] = jnp.broadcast_to(alpha, (1, LANE))
        ab_ref[pl.ds(8 + step, 1), :] = jnp.broadcast_to(beta, (1, LANE))
        inv = 1.0 / beta

        @pl.when(step < STEPS - 1)
        def _():
            norm_and_pack(nxt, inv, True)

        @pl.when(step == STEPS - 1)
        def _():
            norm_and_pack(nxt, inv, False)
        out_copy(nxt, step + 1).start()
        return 0
    ab_ref[...] = jnp.zeros_like(ab_ref)
    lax.fori_loop(0, STEPS, step_body, 0)
    for idx in range(STEPS - 2, STEPS + 1):
        out_copy(idx % 3, idx).wait()


def solution(mesh):
    def local_run(psi_blk, left_env, two_site, right_env):
        slab, s1, s2, bond = psi_blk.shape
        phys = s1 * s2
        terms = left_env.shape[0]
        chunks = bond // LANE
        psi = psi_blk.reshape(slab, phys, bond).transpose(1, 0, 2)
        t = lax.axis_index("terms")
        every_w = lax.all_gather(two_site, "terms", axis=0)
        xn = (1 - t // 2) * 2 + t % 2
        order = jnp.stack([t, t + 1 - 2 * (t % 2), xn, xn + 1 - 2 * (t % 2)])
        w_loc = jnp.take(every_w, order, axis=0)
        eye = jnp.eye(16, dtype=BF)
        kron = (w_loc[:, :, :, None, :, None] * eye[None, None, None, :, None, :]).reshape(4, terms, 16 * phys, 16 * phys)
        any_spec = pl.BlockSpec(memory_space=pl.ANY)
        dma = pltpu.SemaphoreType.DMA
        out, ab, _ = pl.pallas_call(
            lanczos_kernel,
            out_shape=(jax.ShapeDtypeStruct((STEPS + 1, phys, slab, bond), F32),
                       jax.ShapeDtypeStruct((16, LANE), F32),
                       jax.ShapeDtypeStruct((3, terms, bond, bond), BF)),
            in_specs=[any_spec] * 4,
            out_specs=(any_spec, pl.BlockSpec(memory_space=pltpu.VMEM), any_spec),
            scratch_shapes=[
                pltpu.VMEM((3, phys, slab, bond), F32),
                pltpu.VMEM((chunks, phys // 2, bond, 2 * LANE), BF),
                pltpu.VMEM((4, terms, slab, bond), BF),
                pltpu.VMEM((4, terms, 16 * phys, 16 * phys), BF),
                pltpu.VMEM((2, terms, LANE, bond), BF),
                pltpu.VMEM((phys, terms * slab, LANE), BF),
                pltpu.VMEM((phys, slab, terms * LANE), BF),
                pltpu.VMEM((2, 8, 8, LANE), F32),
                pltpu.VMEM((8, LANE), F32),
                dma((3,)), dma((2,)), dma((3,)),
                dma((7, chunks)), dma((7, chunks)), dma((5, chunks)), dma((5, chunks)),
                dma((3,)), dma((3,)), dma((2, 7)), dma((2, 7)),
            ],
            compiler_params=pltpu.CompilerParams(collective_id=0, has_side_effects=True, vmem_limit_bytes=60 * 2**20),
            name="lanczos",
        )(psi, left_env, kron, right_env)
        vectors = out.transpose(0, 2, 1, 3).reshape(STEPS + 1, slab, s1, s2, bond)
        return vectors, ab[:STEPS, 0], ab[8:8 + STEPS, 0]

    return jax.shard_map(local_run, mesh=mesh, in_specs=(P(("rows", "terms")), P("terms", "rows"), P("terms"), P("terms")),
                         out_specs=(P(None, ("rows", "terms")), P(), P()), check_vma=False)
```
